32 devices in a mesh: dp: 2 (over y), space: 16 (over z, x, core).
Axes of the slice: x: 2, y: 2, z: 4, core: 2. Of those that a mesh axis runs over, the one named last changes fastest.
Arguments:
- queries: bfloat16 [16, 200, 256], P('dp'), may hold values from -6 to 6
- query_pos: bfloat16 [200, 256], replicated, may hold values from -6 to 6
- pixels: bfloat16 [16, 4096, 256], P('dp', 'space'), may hold values from -160 to 160
- pixel_pos: bfloat16 [4096, 256], P('space'), may hold values from -6 to 6
- masks: int32 [16, 200, 4096], P('dp', None, 'space'), may hold values from 0 to 1, as said below
- wq_cross: bfloat16 [256, 256], replicated, may hold values from -0.375 to 0.375
- wk_cross: bfloat16 [256, 256], replicated, may hold values from -0.375 to 0.375
- wv_cross: bfloat16 [256, 256], replicated, may hold values from -0.375 to 0.375
- wo_cross: bfloat16 [256, 256], replicated, may hold values from -0.375 to 0.375
- gain_cross: float32 [256], replicated, may hold values from 0.1 to 1.9
- w_qkv: bfloat16 [256, 768], replicated, may hold values from -0.375 to 0.375
- wo_self: bfloat16 [256, 256], replicated, may hold values from -0.375 to 0.375
- gain_self: float32 [256], replicated, may hold values from 0.1 to 1.9
- w_in: bfloat16 [256, 2048], replicated, may hold values from -0.375 to 0.375
- w_out: bfloat16 [2048, 256], replicated, may hold values from -0.125 to 0.125
- gain_ffn: float32 [256], replicated, may hold values from 0.1 to 1.9
Outputs:
- new_queries: bfloat16 [16, 200, 256], P('dp')
The draws below stay inside these ranges and needn't reach their ends.
Inputs may be any that keep to these rules, and one draw needn't show every extreme that they name: `masks`: 0 or 1; each row's ones lie within a run of at most 768 consecutive pixels, which may lie anywhere in the image; a row may have no ones on some devices' pixels or on all pixels of its image.
All inputs are finite; a program needn't handle non-finite values.
Results may differ from the reference program's by a relative error of at most 0.017.
The reference program's roundings to bfloat16 on the way (of `query_in`, `cross_q`, `attended`, `after_cross`, `self_weight`, `self_out`, `after_self` and `hidden`) count: a program that leaves them out, or rounds other values in their place, can miss the bound.
Values may be sent and summed in bfloat16 or wider, within the bound.
A program may use at most 128 MiB of HBM per device.

```python
import jax
import jax.numpy as jnp
from jax import lax

D = 256
HEADS = 8
Q = 200
FF = 2048
IMG_DP = 8
PIX_DEV = 256
IMAGES = 16
PIXELS = 4096


def draw_masks(key, part):
    k_span, k_full, k_start, k_heavy, k_rate, k_empty, k_bits, k_anchor = jax.random.split(jax.random.fold_in(key, 11), 8)
    longest = 3 * PIX_DEV
    spread = PIXELS // PIX_DEV
    row_ids = jnp.arange(Q, dtype=jnp.int32)[None, :, None]
    image_ids = jnp.arange(IMAGES, dtype=jnp.int32)[:, None, None]
    span = jax.random.randint(k_span, (IMAGES, Q, 1), 1, longest + 1)
    full_row = jax.random.randint(k_full, (IMAGES, 1, 1), 0, Q)
    is_full = row_ids == full_row
    span = jnp.where(is_full, longest, span)
    start = jax.random.randint(k_start, (IMAGES, Q, 1), 0, PIXELS - span + 1)
    share = (IMG_DP * Q + spread - 1) // spread
    group_row = image_ids % IMG_DP * Q + row_ids
    far_dev = (group_row // share + spread // 2) % spread
    anchored = jax.random.randint(k_anchor, (IMAGES, Q, 1), 0, 4) == 0
    far_start = jnp.minimum(far_dev * PIX_DEV, PIXELS - span)
    start = jnp.where(anchored, far_start, start)
    heavy_pick = jax.random.randint(k_heavy, (), 0, min(4, IMAGES))
    heavy = image_ids % 4 == heavy_pick
    rate = jnp.where(heavy, 31, jax.random.randint(k_rate, (IMAGES, 1, 1), 0, 33))
    empty = (jax.random.randint(k_empty, (IMAGES, Q, 1), 0, 32) < rate) & jnp.logical_not(is_full) & jnp.logical_not(anchored)
    where_at = jnp.arange(PIXELS, dtype=jnp.int32)[None, None, :]
    ends = (where_at == start) | (where_at == start + span - 1)
    inside = (where_at >= start) & (where_at < start + span)
    bits = (jax.random.randint(k_bits, (IMAGES, Q, PIXELS), 0, 4) > 0) | ends
    keep = inside & bits & jnp.logical_not(empty)
    return keep.astype(jnp.int32)


def draw_pixels(key, part):
    k_base = jax.random.fold_in(jax.random.fold_in(key, 23), 0)
    base = jnp.clip(jax.random.normal(k_base, (IMAGES, PIXELS, D), jnp.float32), -4.0, 4.0)
    return base.astype(jnp.bfloat16)


def shard_levels(stream_key, dims, cuts, low, top_value):
    def one(position, blocks):
        heights = jax.random.uniform(jax.random.fold_in(jax.random.fold_in(stream_key, 6), position), (blocks,), jnp.float32, low / len(cuts), top_value / len(cuts))
        return jnp.repeat(jnp.exp(heights), dims[position] // blocks).reshape((-1,) + (1,) * (len(dims) - position - 1))

    loudness = one(*cuts[0])
    for cut in cuts[1:]:
        loudness = loudness * one(*cut)
    return loudness


def noise(own_key, shape, deviation, reach, shards=(), kind=jnp.bfloat16):
    level = shard_levels(own_key, shape, shards, -0.22, 0.18) if shards else 1.0
    values = jax.random.normal(own_key, shape, jnp.float32) * deviation * level
    return jnp.minimum(jnp.maximum(values, -reach), reach).astype(kind)


def setup_inputs(seed: int = 0) -> dict:
    arg_keys = jax.random.split(jax.random.key(seed), 17)
    return {
        "queries": noise(arg_keys[0], (IMAGES, Q, D), 1.0, 6.0, ((0, 2),)),
        "query_pos": noise(arg_keys[1], (Q, D), 1.0, 6.0),
        "pixels": draw_pixels(jax.random.fold_in(arg_keys[16], 71), 0),
        "pixel_pos": noise(arg_keys[3], (PIXELS, D), 1.0, 6.0, ((0, 16),)),
        "masks": draw_masks(jax.random.fold_in(arg_keys[16], 71), 0),
        "wq_cross": noise(arg_keys[5], (D, D), D ** -0.5, 0.375),
        "wk_cross": noise(arg_keys[6], (D, D), D ** -0.5, 0.375),
        "wv_cross": noise(arg_keys[7], (D, D), D ** -0.5, 0.375),
        "wo_cross": noise(arg_keys[8], (D, D), D ** -0.5, 0.375),
        "gain_cross": jnp.clip(1.0 + 0.18 * jax.random.normal(arg_keys[9], (D,), jnp.float32), 0.1, 1.9),
        "w_qkv": noise(arg_keys[10], (D, 3 * D), D ** -0.5, 0.375),
        "wo_self": noise(arg_keys[11], (D, D), D ** -0.5, 0.375),
        "gain_self": jnp.clip(1.0 + 0.18 * jax.random.normal(arg_keys[12], (D,), jnp.float32), 0.1, 1.9),
        "w_in": noise(arg_keys[13], (D, FF), D ** -0.5, 0.375),
        "w_out": noise(arg_keys[14], (FF, D), FF ** -0.5, 0.125),
        "gain_ffn": jnp.clip(1.0 + 0.18 * jax.random.normal(arg_keys[15], (D,), jnp.float32), 0.1, 1.9),
    }


def layer_norm(x, gain):
    mean = lax.optimization_barrier(jnp.mean(x, axis=-1, keepdims=True))
    var = lax.optimization_barrier(jnp.mean((x - mean) * (x - mean), axis=-1, keepdims=True))
    return (x - mean) / jnp.sqrt(var + 1e-05) * gain

def decoder_rest(queries, attended, query_pos, wo_cross, gain_cross, w_qkv, wo_self, gain_self, w_in, w_out, gain_ffn):
    images, nq, width = queries.shape
    heads = HEADS
    head_size = width // heads
    flat_att = attended.reshape(images * nq, width)
    cross_proj = jnp.dot(flat_att, wo_cross, preferred_element_type=jnp.float32)
    flat_q = queries.reshape(images * nq, width).astype(jnp.float32)
    after_cross = layer_norm(flat_q + cross_proj, gain_cross).astype(jnp.bfloat16)
    pos_rows = jnp.tile(query_pos.astype(jnp.float32), (images, 1))
    self_in = (after_cross.astype(jnp.float32) + pos_rows).astype(jnp.bfloat16)
    both = jnp.dot(self_in, w_qkv[:, :2 * width], preferred_element_type=jnp.float32).astype(jnp.bfloat16)
    self_v = jnp.dot(after_cross, w_qkv[:, 2 * width:], preferred_element_type=jnp.float32).astype(jnp.bfloat16)
    self_q = both[:, :width].reshape(images, nq, heads, head_size)
    self_k = both[:, width:].reshape(images, nq, heads, head_size)
    self_v = self_v.reshape(images, nq, heads, head_size)
    logits = jnp.einsum('iqhd,ikhd->ihqk', self_q.astype(jnp.float32), self_k.astype(jnp.float32)) / jnp.sqrt(jnp.float32(head_size))
    top = lax.optimization_barrier(jnp.max(logits, axis=-1, keepdims=True))
    expo = jnp.exp(logits - top)
    self_weight = (expo / lax.optimization_barrier(jnp.sum(expo, axis=-1, keepdims=True))).astype(jnp.bfloat16)
    self_out = jnp.einsum('ihqk,ikhd->iqhd', self_weight.astype(jnp.float32), self_v.astype(jnp.float32))
    self_out = self_out.astype(jnp.bfloat16).reshape(images * nq, width)
    self_proj = jnp.dot(self_out, wo_self, preferred_element_type=jnp.float32)
    after_self = layer_norm(after_cross.astype(jnp.float32) + self_proj, gain_self).astype(jnp.bfloat16)
    hidden = jnp.maximum(jnp.dot(after_self, w_in, preferred_element_type=jnp.float32), 0.0).astype(jnp.bfloat16)
    ffn_out = jnp.dot(hidden, w_out, preferred_element_type=jnp.float32)
    result = layer_norm(after_self.astype(jnp.float32) + ffn_out, gain_ffn).astype(jnp.bfloat16)
    return result.reshape(images, nq, width)

def reference(queries, query_pos, pixels, pixel_pos, masks, wq_cross, wk_cross, wv_cross, wo_cross, gain_cross, w_qkv, wo_self, gain_self, w_in, w_out, gain_ffn):
    head_size = D // HEADS
    query_in = (queries.astype(jnp.float32) + query_pos.astype(jnp.float32)[None]).astype(jnp.bfloat16)

    def one_image(items):
        qin, pix, mask = items
        cross_q = jnp.dot(qin, wq_cross, preferred_element_type=jnp.float32).astype(jnp.bfloat16).reshape(Q, HEADS, head_size)
        key_in = (pix.astype(jnp.float32) + pixel_pos.astype(jnp.float32)).astype(jnp.bfloat16)
        cross_k = jnp.dot(key_in, wk_cross, preferred_element_type=jnp.float32).astype(jnp.bfloat16).reshape(PIXELS, HEADS, head_size)
        cross_v = jnp.dot(pix, wv_cross, preferred_element_type=jnp.float32).astype(jnp.bfloat16).reshape(PIXELS, HEADS, head_size)
        count = lax.optimization_barrier(jnp.sum(mask, axis=-1))
        allowed = (mask > 0) | (count == 0)[:, None]
        score = jnp.einsum('qhd,phd->qhp', cross_q.astype(jnp.float32), cross_k.astype(jnp.float32)) / jnp.sqrt(jnp.float32(head_size))
        score = jnp.where(allowed[:, None, :], score, -jnp.inf)
        top = lax.optimization_barrier(jnp.max(score, axis=-1, keepdims=True))
        weight = jnp.where(allowed[:, None, :], jnp.exp(score - top), 0.0)
        total = lax.optimization_barrier(jnp.sum(weight, axis=-1))
        summed = jnp.einsum('qhp,phd->qhd', weight.astype(jnp.bfloat16).astype(jnp.float32), cross_v.astype(jnp.float32))
        return (summed / total[..., None]).astype(jnp.bfloat16).reshape(Q, D)
    attended = lax.map(one_image, (query_in, pixels, masks))
    return decoder_rest(queries, attended, query_pos, wo_cross, gain_cross, w_qkv, wo_self, gain_self, w_in, w_out, gain_ffn)
```

```python
import functools

import jax
import jax.numpy as jnp
from jax import lax
from jax.experimental import pallas as pl
from jax.experimental.pallas import tpu as pltpu
from jax.sharding import PartitionSpec as P

HEADS = 8
NEG = -1e30
MESH = pl.DeviceIdType.MESH
F32 = jnp.float32
BF16 = jnp.bfloat16


def nn(a, b):
    return lax.dot_general(a, b, (((1,), (0,)), ((), ())), preferred_element_type=F32)


def nt(a, b):
    return lax.dot_general(a, b, (((1,), (1,)), ((), ())), preferred_element_type=F32)


def eye(size):
    rows = lax.broadcasted_iota(jnp.int32, (size, size), 0)
    cols = lax.broadcasted_iota(jnp.int32, (size, size), 1)
    return jnp.where(rows == cols, 1.0, 0.0).astype(BF16)


def layer_norm(x, gain):
    mean = jnp.mean(x, axis=-1, keepdims=True)
    var = jnp.mean((x - mean) * (x - mean), axis=-1, keepdims=True)
    return (x - mean) / jnp.sqrt(var + 1e-05) * gain


def kernel(
    n,
    queries,
    query_pos,
    pixels,
    pixel_pos,
    masks,
    wq_cross,
    wk_cross,
    wv_cross,
    wo_cross,
    gain_cross,
    w_qkv,
    wo_self,
    gain_self,
    w_in,
    w_out,
    gain_ffn,
    out,
    q_mine,
    q_res,
    qpos_v,
    pix_v,
    pos_v,
    mask_v,
    wq_v,
    wk_v,
    wv_v,
    woc_v,
    gc_v,
    wqkv_v,
    wos_v,
    gs_v,
    win_v,
    wout_v,
    gf_v,
    wqt,
    wvt,
    wvst,
    send_s,
    send_t,
    recv_s,
    recv_t,
    att,
    gath,
    load_sem,
    pix_sem,
    mask_sem,
    xpix_s,
    xpix_r,
    xmask_s,
    xmask_r,
    xpos_s,
    xpos_r,
    ss_sem,
    st_sem,
    rs_sem,
    rt_sem,
    att_s,
    att_r,
    g1_s,
    g2_s,
    g_r,
    out_sem,
):
    images, nq, width = queries.shape
    npix = pixels.shape[1]
    half = images // 2
    npairs = n // 2
    spread = npairs // images
    hp = HEADS // 2
    hd = width // HEADS
    part = width // 2
    scale = 1.4426950408889634 / float(hd) ** 0.5

    me = lax.axis_index("space")
    core = lax.rem(me, 2)
    pair = lax.div(me, 2)
    other = 1 - core
    mate = pair * 2 + other
    base = core * half
    base_other = other * half
    my_image = lax.div(pair, spread)

    def remote(src, dst, ssem, rsem, dev):
        return pltpu.make_async_remote_copy(
            src_ref=src,
            dst_ref=dst,
            send_sem=ssem,
            recv_sem=rsem,
            device_id={"space": dev},
            device_id_type=MESH,
        )

    barrier = pltpu.get_barrier_semaphore()

    def greet(k, carry):
        dev = lax.rem(me + k, n)
        pl.semaphore_signal(barrier, inc=1, device_id={"space": dev}, device_id_type=MESH)
        return carry

    lax.fori_loop(1, n, greet, 0)

    loads = [
        (query_pos, qpos_v),
        (queries.at[pl.ds(base, half)], q_mine),
        (wq_cross, wq_v),
        (wk_cross, wk_v),
        (wv_cross, wv_v),
        (pixel_pos, pos_v.at[0]),
        (queries.at[my_image], q_res),
        (wo_cross, woc_v),
        (gain_cross, gc_v),
        (w_qkv, wqkv_v),
        (wo_self, wos_v),
        (gain_self, gs_v),
        (w_in, win_v),
        (w_out, wout_v),
        (gain_ffn, gf_v),
    ]
    load = [pltpu.make_async_copy(s, d, load_sem.at[i]) for i, (s, d) in enumerate(loads)]
    for c in load[:6]:
        c.start()
    pix_own = pltpu.make_async_copy(pixels.at[pl.ds(base, half)], pix_v.at[0], pix_sem)
    mask_own = pltpu.make_async_copy(masks.at[pl.ds(base, half)], mask_v.at[0], mask_sem)
    pix_own.start()
    mask_own.start()

    ident = eye(npix)
    for c in load[:6]:
        c.wait()
    wqt[...] = nt(eye(width), wq_v[...]).astype(BF16)
    wvt[...] = nt(eye(width), wv_v[...]).astype(BF16)

    pl.semaphore_wait(barrier, n - 1)
    xpos = remote(pixel_pos, pos_v.at[1], xpos_s, xpos_r, mate)
    xpos.start()

    def xpix(j):
        return remote(
            pixels.at[base_other + j], pix_v.at[1, j], xpix_s.at[j], xpix_r.at[j], mate
        )

    def xmask(j):
        return remote(
            masks.at[base_other + j], mask_v.at[1, j], xmask_s.at[j], xmask_r.at[j], mate
        )

    for j in range(half):
        xmask(j).start()
        xpix(j).start()
    for c in load[6:]:
        c.start()
    pix_own.wait()
    mask_own.wait()
    xpos.wait()

    def send_s_copy(j, o):
        owner = (base + j) * spread * 2 + o
        return owner, remote(
            send_s.at[j, o], recv_s.at[pair], ss_sem.at[j, o], rs_sem.at[pair], owner
        )

    def send_t_copy(j, o):
        owner = (base + j) * spread * 2 + o
        return owner, remote(
            send_t.at[j, o], recv_t.at[pair], st_sem.at[j, o], rt_sem.at[pair], owner
        )

    def one_image(j, carry):
        xmask(j).wait()
        xpix(j).wait()
        qin = (q_mine[j].astype(F32) + qpos_v[...].astype(F32)).astype(BF16)
        cqt = nt(wqt[...], qin).astype(BF16)
        keys, values, seen = [], [], []
        for side in range(2):
            pix = pix_v[side, j]
            key_in = (pix.astype(F32) + pos_v[side].astype(F32)).astype(BF16)
            keys.append(nn(key_in, wk_v[...]).astype(BF16))
            values.append(nt(wvt[...], pix).astype(BF16))
            seen.append(nt(ident, mask_v[side, j].astype(F32).astype(BF16)))
        key = jnp.concatenate(keys, axis=0)
        value = jnp.concatenate(values, axis=1)
        seen = jnp.concatenate(seen, axis=0)
        found = jnp.max(seen, axis=0, keepdims=True)
        bias = jnp.where(jnp.logical_or(seen > 0.5, found < 0.5), 0.0, NEG)
        for h in range(HEADS):
            pieces = [cqt[h * hd : (h + 1) * hd]]
            if h:
                pieces.insert(0, jnp.zeros((h * hd, nq), BF16))
            if h < HEADS - 1:
                pieces.append(jnp.zeros((width - (h + 1) * hd, nq), BF16))
            score = nn(key, jnp.concatenate(pieces, axis=0)) + bias
            top = jnp.max(score, axis=0, keepdims=True)
            weight = jnp.exp2((score - top) * scale)
            total = jnp.sum(weight, axis=0, keepdims=True)
            summed = nn(value[h * hd : (h + 1) * hd], weight.astype(BF16))
            o, r = h // hp, h % hp
            send_s[j, o, r * hd : (r + 1) * hd, :] = summed.astype(BF16)
            send_t[j, o, r : r + 1, :] = top
            send_t[j, o, hp + r : hp + r + 1, :] = total
        for o in range(2):
            send_t[j, o, 2 * hp : 2 * hp + 1, :] = found
        for o in range(2):
            owner, copy_s = send_s_copy(j, o)
            _, copy_t = send_t_copy(j, o)

            @pl.when(owner != me)
            def _():
                copy_t.start()
                copy_s.start()

            @pl.when(owner == me)
            def _():
                pltpu.make_async_copy(send_t.at[j, o], recv_t.at[pair], rt_sem.at[pair]).start()
                pltpu.make_async_copy(send_s.at[j, o], recv_s.at[pair], rs_sem.at[pair]).start()

        return carry

    lax.fori_loop(0, half, one_image, 0)

    for c in load[6:]:
        c.wait()
    wvst[...] = nt(eye(width), wqkv_v[:, 2 * width :]).astype(BF16)

    def fold(k, carry):
        top, total, flag, acc = carry
        slot = lax.rem(pair + k, npairs)
        pltpu.make_async_copy(recv_t.at[slot], recv_t.at[slot], rt_sem.at[slot]).wait()
        pltpu.make_async_copy(recv_s.at[slot], recv_s.at[slot], rs_sem.at[slot]).wait()
        new_top = recv_t[slot, 0:hp, :]
        new_total = recv_t[slot, hp : 2 * hp, :]
        new_flag = recv_t[slot, 2 * hp : 2 * hp + 1, :]
        new = recv_s[slot].astype(F32)
        best = jnp.maximum(flag, new_flag)
        a = jnp.where(flag == best, top, NEG)
        b = jnp.where(new_flag == best, new_top, NEG)
        top = jnp.maximum(a, b)
        ea = jnp.exp2((a - top) * scale)
        eb = jnp.exp2((b - top) * scale)
        total = total * ea + new_total * eb
        acc = jnp.concatenate(
            [
                acc[r * hd : (r + 1) * hd] * ea[r : r + 1] + new[r * hd : (r + 1) * hd] * eb[r : r + 1]
                for r in range(hp)
            ],
            axis=0,
        )
        return top, total, best, acc

    def gather_copy(ssem, image, c, dev):
        ref = gath.at[image, c]
        return remote(ref, ref, ssem, g_r.at[image, c], dev)

    def owner_work():
        start = (
            jnp.full((hp, nq), NEG, F32),
            jnp.zeros((hp, nq), F32),
            jnp.full((1, nq), -1.0, F32),
            jnp.zeros((part, nq), F32),
        )
        top, total, flag, acc = lax.fori_loop(0, npairs, fold, start)
        mine = jnp.concatenate(
            [acc[r * hd : (r + 1) * hd] / total[r : r + 1] for r in range(hp)], axis=0
        ).astype(BF16)
        att[core] = mine
        swap = remote(att.at[core], att.at[core], att_s, att_r.at[core], mate)
        swap.start()
        pltpu.make_async_copy(att.at[other], att.at[other], att_r.at[other]).wait()
        attended_t = jnp.concatenate([att[0], att[1]], axis=0)
        ident_q = eye(nq)
        attended = nt(ident_q, attended_t).astype(BF16)
        cross_proj = nn(attended, woc_v[...])
        after_cross = layer_norm(q_res[...].astype(F32) + cross_proj, gc_v[...]).astype(BF16)
        ac32 = after_cross.astype(F32)
        self_in = (ac32 + qpos_v[...].astype(F32)).astype(BF16)
        both = nn(self_in, wqkv_v[:, : 2 * width]).astype(BF16)
        sq, sk = both[:, :width], both[:, width:]
        svt = nt(wvst[...], after_cross).astype(BF16)
        lane_head = lax.broadcasted_iota(jnp.int32, (nq, width), 1) // hd
        outs = []
        for h in range(HEADS):
            key = jnp.where(lane_head == h, sk.astype(F32), 0.0).astype(BF16)
            logits = nt(key, sq)
            top = jnp.max(logits, axis=0, keepdims=True)
            expo = jnp.exp2((logits - top) * scale)
            weight = (expo / jnp.sum(expo, axis=0, keepdims=True)).astype(BF16)
            outs.append(nn(svt[h * hd : (h + 1) * hd], weight).astype(BF16))
        self_out = nt(ident_q, jnp.concatenate(outs, axis=0)).astype(BF16)
        self_proj = nn(self_out, wos_v[...])
        after_self = layer_norm(ac32 + self_proj, gs_v[...]).astype(BF16)
        hidden = jnp.maximum(nn(after_self, win_v[...]), 0.0).astype(BF16)
        ffn = nn(hidden, wout_v[...])
        result = layer_norm(after_self.astype(F32) + ffn, gf_v[...]).astype(BF16)
        for c in range(2):
            gath[my_image, c] = result[:, c * part : (c + 1) * part]

        def spread_out(k, carry):
            dev = lax.rem(pair + k, npairs) * 2 + core
            gather_copy(g1_s.at[k], my_image, core, dev).start()
            return carry

        lax.fori_loop(1, npairs, spread_out, 0)
        swap.wait_send()

    is_owner = lax.rem(pair, spread) == 0
    if spread == 1:
        owner_work()
    else:
        pl.when(is_owner)(owner_work)

    def write_out(image, c):
        return pltpu.make_async_copy(
            gath.at[image, c],
            out.at[image, :, pl.ds(pl.multiple_of(c * part, part), part)],
            out_sem.at[image, c],
        )

    def arrive_near(k, carry):
        image = lax.rem(my_image + k, images)
        not_mine = jnp.logical_or(image != my_image, jnp.logical_not(is_owner))

        @pl.when(not_mine)
        def _():
            ref = gath.at[image, core]
            pltpu.make_async_copy(ref, ref, g_r.at[image, core]).wait()
            gather_copy(g2_s.at[image], image, core, mate).start()

        write_out(image, core).start()
        return carry

    lax.fori_loop(0, images, arrive_near, 0)

    def arrive_far(k, carry):
        image = lax.rem(my_image + k, images)
        not_mine = jnp.logical_or(image != my_image, jnp.logical_not(is_owner))

        @pl.when(not_mine)
        def _():
            ref = gath.at[image, other]
            pltpu.make_async_copy(ref, ref, g_r.at[image, other]).wait()

        write_out(image, other).start()
        return carry

    lax.fori_loop(0, images, arrive_far, 0)

    def drain_sends(j, carry):
        for o in range(2):
            owner, copy_s = send_s_copy(j, o)
            _, copy_t = send_t_copy(j, o)

            @pl.when(owner != me)
            def _():
                copy_s.wait_send()
                copy_t.wait_send()

        return carry

    lax.fori_loop(0, half, drain_sends, 0)

    def drain_spread():
        def body(k, carry):
            dev = lax.rem(pair + k, npairs) * 2 + core
            gather_copy(g1_s.at[k], my_image, core, dev).wait_send()
            return carry

        lax.fori_loop(1, npairs, body, 0)

    if spread == 1:
        drain_spread()
    else:
        pl.when(is_owner)(drain_spread)

    def drain_out(image, carry):
        not_mine = jnp.logical_or(image != my_image, jnp.logical_not(is_owner))

        @pl.when(not_mine)
        def _():
            gather_copy(g2_s.at[image], image, core, mate).wait_send()

        for c in range(2):
            write_out(image, c).wait()
        return carry

    lax.fori_loop(0, images, drain_out, 0)


def local(n, *args):
    queries, query_pos, pixels, pixel_pos, masks = args[:5]
    args = list(args)
    for i in (9, 12, 15):
        args[i] = args[i].reshape(1, -1)
    images, nq, width = queries.shape
    npix = pixels.shape[1]
    half = images // 2
    npairs = n // 2
    part = width // 2
    hp = HEADS // 2
    ff = args[13].shape[1]
    dma = pltpu.SemaphoreType.DMA
    scratch = [
        pltpu.VMEM((half, nq, width), BF16),
        pltpu.VMEM((nq, width), BF16),
        pltpu.VMEM((nq, width), BF16),
        pltpu.VMEM((2, half, npix, width), BF16),
        pltpu.VMEM((2, npix, width), BF16),
        pltpu.VMEM((2, half, nq, npix), jnp.int32),
        pltpu.VMEM((width, width), BF16),
        pltpu.VMEM((width, width), BF16),
        pltpu.VMEM((width, width), BF16),
        pltpu.VMEM((width, width), BF16),
        pltpu.VMEM((1, width), F32),
        pltpu.VMEM((width, 3 * width), BF16),
        pltpu.VMEM((width, width), BF16),
        pltpu.VMEM((1, width), F32),
        pltpu.VMEM((width, ff), BF16),
        pltpu.VMEM((ff, width), BF16),
        pltpu.VMEM((1, width), F32),
        pltpu.VMEM((width, width), BF16),
        pltpu.VMEM((width, width), BF16),
        pltpu.VMEM((width, width), BF16),
        pltpu.VMEM((half, 2, part, nq), BF16),
        pltpu.VMEM((half, 2, 2 * hp + 1, nq), F32),
        pltpu.VMEM((npairs, part, nq), BF16),
        pltpu.VMEM((npairs, 2 * hp + 1, nq), F32),
        pltpu.VMEM((2, part, nq), BF16),
        pltpu.VMEM((images, 2, nq, part), BF16),
        dma((15,)),
        dma,
        dma,
        dma((half,)),
        dma((half,)),
        dma((half,)),
        dma((half,)),
        dma,
        dma,
        dma((half, 2)),
        dma((half, 2)),
        dma((npairs,)),
        dma((npairs,)),
        dma,
        dma((2,)),
        dma((npairs,)),
        dma((images,)),
        dma((images, 2)),
        dma((images, 2)),
    ]
    return pl.pallas_call(
        functools.partial(kernel, n),
        out_shape=jax.ShapeDtypeStruct((images, nq, width), BF16),
        in_specs=[pl.BlockSpec(memory_space=pl.ANY)] * len(args),
        out_specs=pl.BlockSpec(memory_space=pl.ANY),
        scratch_shapes=scratch,
        compiler_params=pltpu.CompilerParams(
            collective_id=0, has_side_effects=True, vmem_limit_bytes=60 * 1024 * 1024
        ),
    )(*args)


def solution(mesh):
    placed = (
        P("dp", None, None),
        P(),
        P("dp", "space", None),
        P("space", None),
        P("dp", None, "space"),
    ) + (P(),) * 11
    return jax.shard_map(
        functools.partial(local, mesh.shape["space"]),
        mesh=mesh,
        in_specs=placed,
        out_specs=P("dp", None, None),
        check_vma=False,
    )
```

```python
import functools

import jax
import jax.numpy as jnp
from jax import lax
from jax.experimental import pallas as pl
from jax.experimental.pallas import tpu as pltpu
from jax.sharding import PartitionSpec as P

HEADS = 8
NEG = -1e30
MESH = pl.DeviceIdType.MESH
F32 = jnp.float32
BF16 = jnp.bfloat16


def nn(a, b):
    return lax.dot_general(a, b, (((1,), (0,)), ((), ())), preferred_element_type=F32)


def nt(a, b):
    return lax.dot_general(a, b, (((1,), (1,)), ((), ())), preferred_element_type=F32)


def eye(size):
    rows = lax.broadcasted_iota(jnp.int32, (size, size), 0)
    cols = lax.broadcasted_iota(jnp.int32, (size, size), 1)
    return jnp.where(rows == cols, 1.0, 0.0).astype(BF16)


def layer_norm(x, gain):
    mean = jnp.mean(x, axis=-1, keepdims=True)
    var = jnp.mean((x - mean) * (x - mean), axis=-1, keepdims=True)
    return (x - mean) / jnp.sqrt(var + 1e-05) * gain


def kernel(
    n,
    queries,
    query_pos,
    pixels,
    pixel_pos,
    masks,
    wq_cross,
    wk_cross,
    wv_cross,
    wo_cross,
    gain_cross,
    w_qkv,
    wo_self,
    gain_self,
    w_in,
    w_out,
    gain_ffn,
    out,
    q_mine,
    q_res,
    qpos_v,
    pix_v,
    pos_v,
    mask_v,
    wq_v,
    wk_v,
    wv_v,
    woc_v,
    gc_v,
    wqkv_v,
    wos_v,
    gs_v,
    win_v,
    wout_v,
    gf_v,
    wkt,
    wvst,
    key_v,
    val_v,
    cq_v,
    send_s,
    send_t,
    send_f,
    recv_s,
    recv_t,
    recv_f,
    att,
    gath,
    load_sem,
    pix_sem,
    mask_sem,
    xpix_s,
    xpix_r,
    xmask_s,
    xmask_r,
    xpos_s,
    xpos_r,
    ss_sem,
    st_sem,
    sf_sem,
    rs_sem,
    rt_sem,
    rf_sem,
    att_s,
    att_r,
    g1_s,
    g2_s,
    g3_s,
    g_r,
    out_sem,
):
    images, nq, width = queries.shape
    npix = pixels.shape[1]
    half = images // 2
    npairs = n // 2
    spread = npairs // images
    hp = HEADS // 2
    hd = width // HEADS
    part = width // 2
    scale = 1.4426950408889634 / float(hd) ** 0.5

    me = lax.axis_index("space")
    core = lax.rem(me, 2)
    pair = lax.div(me, 2)
    other = 1 - core
    mate = pair * 2 + other
    base = core * half
    base_other = other * half
    my_image = lax.div(pair, spread)

    def remote(src, dst, ssem, rsem, dev):
        return pltpu.make_async_remote_copy(
            src_ref=src,
            dst_ref=dst,
            send_sem=ssem,
            recv_sem=rsem,
            device_id={"space": dev},
            device_id_type=MESH,
        )

    barrier = pltpu.get_barrier_semaphore()

    def greet(k, carry):
        dev = lax.rem(me + k, n)
        pl.semaphore_signal(barrier, inc=1, device_id={"space": dev}, device_id_type=MESH)
        return carry

    lax.fori_loop(1, n, greet, 0)

    loads = [
        (query_pos, qpos_v),
        (queries.at[pl.ds(base, half)], q_mine),
        (wq_cross, wq_v),
        (wk_cross, wk_v),
        (wv_cross, wv_v),
        (pixel_pos, pos_v.at[0]),
        (queries.at[my_image], q_res),
        (wo_cross, woc_v),
        (gain_cross, gc_v),
        (w_qkv, wqkv_v),
        (wo_self, wos_v),
        (gain_self, gs_v),
        (w_in, win_v),
        (w_out, wout_v),
        (gain_ffn, gf_v),
    ]
    load = [pltpu.make_async_copy(s, d, load_sem.at[i]) for i, (s, d) in enumerate(loads)]
    for c in load[:6]:
        c.start()
    pix_own = pltpu.make_async_copy(pixels.at[pl.ds(base, half)], pix_v.at[0], pix_sem)
    mask_own = pltpu.make_async_copy(masks.at[pl.ds(base, half)], mask_v.at[0], mask_sem)
    pix_own.start()
    mask_own.start()

    for c in load[:6]:
        c.wait()
    wkt[...] = nt(eye(width), wk_v[...]).astype(BF16)

    pl.semaphore_wait(barrier, n - 1)
    xpos = remote(pixel_pos, pos_v.at[1], xpos_s, xpos_r, mate)
    xpos.start()

    def xpix(j):
        return remote(
            pixels.at[base_other + j], pix_v.at[1, j], xpix_s.at[j], xpix_r.at[j], mate
        )

    def xmask(j):
        return remote(
            masks.at[base_other + j], mask_v.at[1, j], xmask_s.at[j], xmask_r.at[j], mate
        )

    for jj in range(half):
        xmask(lax.rem(jj + pair, half)).start()
        xpix(lax.rem(jj + pair, half)).start()
    for c in load[6:]:
        c.start()
    pix_own.wait()
    mask_own.wait()

    lane_head = lax.broadcasted_iota(jnp.int32, (nq, width), 1) // hd
    lane = lax.broadcasted_iota(jnp.int32, (nq, 128), 1)

    def project(side, j):
        pix = pix_v[side, j]
        key_in = (pix.astype(F32) + pos_v[side].astype(F32)).astype(BF16)
        key_t = nt(wkt[...], key_in).astype(BF16)
        value = nn(pix, wv_v[...]).astype(BF16)
        return key_t, value

    def own_side(j, carry):
        qin = (q_mine[j].astype(F32) + qpos_v[...].astype(F32)).astype(BF16)
        cq_v[j] = nn(qin, wq_v[...]).astype(BF16)
        key_v[j], val_v[j] = project(0, j)
        return carry

    lax.fori_loop(0, half, own_side, 0)
    xpos.wait()

    def send_copies(j, o):
        owner = (base + j) * spread * 2 + o
        return owner, (
            remote(send_f.at[j], recv_f.at[pair], sf_sem.at[j, o], rf_sem.at[pair], owner),
            remote(send_t.at[j, o], recv_t.at[pair], st_sem.at[j, o], rt_sem.at[pair], owner),
            remote(send_s.at[j, o], recv_s.at[pair], ss_sem.at[j, o], rs_sem.at[pair], owner),
        )

    def one_image(jj, carry):
        j = lax.rem(jj + pair, half)
        xmask(j).wait()
        xpix(j).wait()
        cq = cq_v[j].astype(F32)
        key, value = project(1, j)
        key = jnp.concatenate([key_v[j], key], axis=1)
        value = jnp.concatenate([val_v[j], value], axis=0)
        seen = jnp.concatenate([mask_v[0, j], mask_v[1, j]], axis=1).astype(F32)
        found = jnp.max(seen, axis=1, keepdims=True)
        bias = jnp.where(jnp.logical_or(seen > 0.5, found < 0.5), 0.0, NEG)
        stats = jnp.where(lane == 4 * hp, found, 0.0)
        rows = jnp.zeros((nq, width), F32)
        for h in range(HEADS):
            query = jnp.where(lane_head == h, cq, 0.0).astype(BF16)
            score = nn(query, key) + bias
            top = jnp.max(score, axis=1, keepdims=True)
            weight = jnp.exp2((score - top) * scale)
            total = jnp.sum(weight, axis=1, keepdims=True)
            rows = jnp.where(lane_head == h, nn(weight.astype(BF16), value), rows)
            o, r = h // hp, h % hp
            stats = jnp.where(lane == o * 2 * hp + r, top, stats)
            stats = jnp.where(lane == o * 2 * hp + hp + r, total, stats)
        rows = rows.astype(BF16)
        stats = jnp.transpose(stats)
        for o in range(2):
            send_t[j, o] = stats[o * 2 * hp : (o + 1) * 2 * hp]
        send_f[j] = stats[4 * hp : 4 * hp + 1]
        for o in range(2):
            send_s[j, o] = rows[:, o * part : (o + 1) * part]
        for o in range(2):
            owner, copies = send_copies(j, o)

            @pl.when(owner != me)
            def _():
                for copy in copies:
                    copy.start()

            @pl.when(owner == me)
            def _():
                here = pltpu.make_async_copy
                here(send_f.at[j], recv_f.at[pair], rf_sem.at[pair]).start()
                here(send_t.at[j, o], recv_t.at[pair], rt_sem.at[pair]).start()
                here(send_s.at[j, o], recv_s.at[pair], rs_sem.at[pair]).start()

        return carry

    lax.fori_loop(0, half, one_image, 0)

    for c in load[6:]:
        c.wait()
    wvst[...] = nt(eye(width), wqkv_v[:, 2 * width :]).astype(BF16)

    ident_p = eye(part)

    def fold(k, carry):
        top, total, flag, acc = carry
        slot = lax.rem(pair + k, npairs)
        pltpu.make_async_copy(recv_f.at[slot], recv_f.at[slot], rf_sem.at[slot]).wait()
        pltpu.make_async_copy(recv_t.at[slot], recv_t.at[slot], rt_sem.at[slot]).wait()
        pltpu.make_async_copy(recv_s.at[slot], recv_s.at[slot], rs_sem.at[slot]).wait()
        new_top = recv_t[slot, 0:hp, :]
        new_total = recv_t[slot, hp : 2 * hp, :]
        new_flag = recv_f[slot]
        new = nt(ident_p, recv_s[slot])
        best = jnp.maximum(flag, new_flag)
        a = jnp.where(flag == best, top, NEG)
        b = jnp.where(new_flag == best, new_top, NEG)
        top = jnp.maximum(a, b)
        ea = jnp.exp2((a - top) * scale)
        eb = jnp.exp2((b - top) * scale)
        total = total * ea + new_total * eb
        acc = jnp.concatenate(
            [
                acc[r * hd : (r + 1) * hd] * ea[r : r + 1] + new[r * hd : (r + 1) * hd] * eb[r : r + 1]
                for r in range(hp)
            ],
            axis=0,
        )
        return top, total, best, acc

    def gather_copy(ssem, image, c, dev):
        ref = gath.at[image, c]
        return remote(ref, ref, ssem, g_r.at[image, c], dev)

    relay = spread == 1 and npairs % 2 == 0
    step = 2 if relay else 1
    pair_across = pair + 1 - 2 * lax.rem(pair, 2)
    across = pair_across * 2 + core

    def owner_work():
        start = (
            jnp.full((hp, nq), NEG, F32),
            jnp.zeros((hp, nq), F32),
            jnp.full((1, nq), -1.0, F32),
            jnp.zeros((part, nq), F32),
        )
        top, total, flag, acc = lax.fori_loop(0, npairs, fold, start)
        mine = jnp.concatenate(
            [acc[r * hd : (r + 1) * hd] / total[r : r + 1] for r in range(hp)], axis=0
        ).astype(BF16)
        att[core] = mine
        swap = remote(att.at[core], att.at[core], att_s, att_r.at[core], mate)
        swap.start()
        pltpu.make_async_copy(att.at[other], att.at[other], att_r.at[other]).wait()
        attended_t = jnp.concatenate([att[0], att[1]], axis=0)
        ident_q = eye(nq)
        attended = nt(ident_q, attended_t).astype(BF16)
        cross_proj = nn(attended, woc_v[...])
        after_cross = layer_norm(q_res[...].astype(F32) + cross_proj, gc_v[...]).astype(BF16)
        ac32 = after_cross.astype(F32)
        self_in = (ac32 + qpos_v[...].astype(F32)).astype(BF16)
        both = nn(self_in, wqkv_v[:, : 2 * width]).astype(BF16)
        sq, sk = both[:, :width], both[:, width:]
        svt = nt(wvst[...], after_cross).astype(BF16)
        outs = []
        for h in range(HEADS):
            key = jnp.where(lane_head == h, sk.astype(F32), 0.0).astype(BF16)
            logits = nt(key, sq)
            top = jnp.max(logits, axis=0, keepdims=True)
            expo = jnp.exp2((logits - top) * scale)
            weight = (expo / jnp.sum(expo, axis=0, keepdims=True)).astype(BF16)
            outs.append(nn(svt[h * hd : (h + 1) * hd], weight).astype(BF16))
        self_out = nt(ident_q, jnp.concatenate(outs, axis=0)).astype(BF16)
        self_proj = nn(self_out, wos_v[...])
        after_self = layer_norm(ac32 + self_proj, gs_v[...]).astype(BF16)
        hidden = jnp.maximum(nn(after_self, win_v[...]), 0.0).astype(BF16)
        ffn = nn(hidden, wout_v[...])
        result = layer_norm(after_self.astype(F32) + ffn, gf_v[...]).astype(BF16)
        for c in range(2):
            gath[my_image, c] = result[:, c * part : (c + 1) * part]

        if relay:
            gather_copy(g3_s.at[my_image], my_image, core, across).start()

        def spread_out(k, carry):
            k = k * step
            dev = lax.rem(pair + k, npairs) * 2 + core
            gather_copy(g1_s.at[k], my_image, core, dev).start()
            return carry

        lax.fori_loop(1, npairs // step, spread_out, 0)
        swap.wait_send()

    is_owner = lax.rem(pair, spread) == 0
    if spread == 1:
        owner_work()
    else:
        pl.when(is_owner)(owner_work)

    def write_out(image, c):
        return pltpu.make_async_copy(
            gath.at[image, c],
            out.at[image, :, pl.ds(pl.multiple_of(c * part, part), part)],
            out_sem.at[image, c],
        )

    def arrived(image, c):
        ref = gath.at[image, c]
        pltpu.make_async_copy(ref, ref, g_r.at[image, c]).wait()

    def relayed():
        for c in range(2):
            write_out(my_image, c).start()

        def direct(k, carry):
            image = lax.rem(pair + 2 * k, images)
            arrived(image, core)
            gather_copy(g3_s.at[image], image, core, across).start()
            gather_copy(g2_s.at[image], image, core, mate).start()
            write_out(image, core).start()
            return carry

        def second(k, carry):
            image = lax.rem(pair_across + 2 * k, images)
            arrived(image, core)
            gather_copy(g2_s.at[image], image, core, mate).start()
            write_out(image, core).start()
            return carry

        def third(k, carry):
            image = lax.rem(pair + k, images)
            arrived(image, other)
            write_out(image, other).start()
            return carry

        lax.fori_loop(1, images // 2, direct, 0)
        lax.fori_loop(0, images // 2, second, 0)
        lax.fori_loop(1, images, third, 0)

    def plain():
        def arrive_near(k, carry):
            image = lax.rem(my_image + k, images)
            not_mine = jnp.logical_or(image != my_image, jnp.logical_not(is_owner))

            @pl.when(not_mine)
            def _():
                ref = gath.at[image, core]
                pltpu.make_async_copy(ref, ref, g_r.at[image, core]).wait()
                gather_copy(g2_s.at[image], image, core, mate).start()

            write_out(image, core).start()
            return carry

        lax.fori_loop(0, images, arrive_near, 0)

        def arrive_far(k, carry):
            image = lax.rem(my_image + k, images)
            not_mine = jnp.logical_or(image != my_image, jnp.logical_not(is_owner))

            @pl.when(not_mine)
            def _():
                ref = gath.at[image, other]
                pltpu.make_async_copy(ref, ref, g_r.at[image, other]).wait()

            write_out(image, other).start()
            return carry

        lax.fori_loop(0, images, arrive_far, 0)

    if relay:
        relayed()
    else:
        plain()

    def drain_sends(j, carry):
        for o in range(2):
            owner, copies = send_copies(j, o)

            @pl.when(owner != me)
            def _():
                for copy in copies:
                    copy.wait_send()

        return carry

    lax.fori_loop(0, half, drain_sends, 0)

    def drain_spread():
        def body(k, carry):
            k = k * step
            dev = lax.rem(pair + k, npairs) * 2 + core
            gather_copy(g1_s.at[k], my_image, core, dev).wait_send()
            return carry

        lax.fori_loop(1, npairs // step, body, 0)
        if relay:

            def across_body(k, carry):
                image = lax.rem(pair + 2 * k, images)
                gather_copy(g3_s.at[image], image, core, across).wait_send()
                return carry

            lax.fori_loop(0, images // 2, across_body, 0)

    if spread == 1:
        drain_spread()
    else:
        pl.when(is_owner)(drain_spread)

    def drain_out(image, carry):
        not_mine = jnp.logical_or(image != my_image, jnp.logical_not(is_owner))

        @pl.when(not_mine)
        def _():
            gather_copy(g2_s.at[image], image, core, mate).wait_send()

        for c in range(2):
            write_out(image, c).wait()
        return carry

    lax.fori_loop(0, images, drain_out, 0)


def local(n, *args):
    queries, query_pos, pixels, pixel_pos, masks = args[:5]
    args = list(args)
    for i in (9, 12, 15):
        args[i] = args[i].reshape(1, -1)
    images, nq, width = queries.shape
    npix = pixels.shape[1]
    half = images // 2
    npairs = n // 2
    part = width // 2
    hp = HEADS // 2
    ff = args[13].shape[1]
    dma = pltpu.SemaphoreType.DMA
    scratch = [
        pltpu.VMEM((half, nq, width), BF16),
        pltpu.VMEM((nq, width), BF16),
        pltpu.VMEM((nq, width), BF16),
        pltpu.VMEM((2, half, npix, width), BF16),
        pltpu.VMEM((2, npix, width), BF16),
        pltpu.VMEM((2, half, nq, npix), jnp.int32),
        pltpu.VMEM((width, width), BF16),
        pltpu.VMEM((width, width), BF16),
        pltpu.VMEM((width, width), BF16),
        pltpu.VMEM((width, width), BF16),
        pltpu.VMEM((1, width), F32),
        pltpu.VMEM((width, 3 * width), BF16),
        pltpu.VMEM((width, width), BF16),
        pltpu.VMEM((1, width), F32),
        pltpu.VMEM((width, ff), BF16),
        pltpu.VMEM((ff, width), BF16),
        pltpu.VMEM((1, width), F32),
        pltpu.VMEM((width, width), BF16),
        pltpu.VMEM((width, width), BF16),
        pltpu.VMEM((half, width, npix), BF16),
        pltpu.VMEM((half, npix, width), BF16),
        pltpu.VMEM((half, nq, width), BF16),
        pltpu.VMEM((half, 2, nq, part), BF16),
        pltpu.VMEM((half, 2, 2 * hp, nq), F32),
        pltpu.VMEM((half, 1, nq), F32),
        pltpu.VMEM((npairs, nq, part), BF16),
        pltpu.VMEM((npairs, 2 * hp, nq), F32),
        pltpu.VMEM((npairs, 1, nq), F32),
        pltpu.VMEM((2, part, nq), BF16),
        pltpu.VMEM((images, 2, nq, part), BF16),
        dma((15,)),
        dma,
        dma,
        dma((half,)),
        dma((half,)),
        dma((half,)),
        dma((half,)),
        dma,
        dma,
        dma((half, 2)),
        dma((half, 2)),
        dma((half, 2)),
        dma((npairs,)),
        dma((npairs,)),
        dma((npairs,)),
        dma,
        dma((2,)),
        dma((npairs,)),
        dma((images,)),
        dma((images,)),
        dma((images, 2)),
        dma((images, 2)),
    ]
    return pl.pallas_call(
        functools.partial(kernel, n),
        out_shape=jax.ShapeDtypeStruct((images, nq, width), BF16),
        in_specs=[pl.BlockSpec(memory_space=pl.ANY)] * len(args),
        out_specs=pl.BlockSpec(memory_space=pl.ANY),
        scratch_shapes=scratch,
        compiler_params=pltpu.CompilerParams(
            collective_id=0, has_side_effects=True, vmem_limit_bytes=60 * 1024 * 1024
        ),
    )(*args)


def solution(mesh):
    placed = (
        P("dp", None, None),
        P(),
        P("dp", "space", None),
        P("space", None),
        P("dp", None, "space"),
    ) + (P(),) * 11
    return jax.shard_map(
        functools.partial(local, mesh.shape["space"]),
        mesh=mesh,
        in_specs=placed,
        out_specs=P("dp", None, None),
        check_vma=False,
    )
```
